16 devices in a mesh: dp: 4 (over y, z, core), tp: 4 (over x).
Axes of the slice: x: 4, y: 2, z: 1, core: 2. Of those that a mesh axis runs over, the one named last changes fastest.
The devices are a block of a 4x4x8 slice.
Arguments:
- x: bfloat16 [8192, 2048], P(('dp', 'tp')), parts along dimension 0
- dy: bfloat16 [8192, 2048], P(('dp', 'tp')), parts along dimension 0
- gain: bfloat16 [2048], replicated
- wq: bfloat16 [2048, 4096], P(None, 'tp')
- wk: bfloat16 [2048, 2048], P(None, 'tp')
- wv: bfloat16 [2048, 2048], P(None, 'tp')
- wo: bfloat16 [4096, 2048], P('tp')
Outputs:
- output 1: bfloat16 [8192, 2048], P(('dp', 'tp')), parts along dimension 0
- output 2: float32 [4, 2048], P('dp'), parts along dimension 0
- output 3: bfloat16 [8192, 4096], P('dp', 'tp'), parts along dimension 0
- output 4: bfloat16 [8192, 2048], P('dp', 'tp'), parts along dimension 0
- output 5: bfloat16 [8192, 2048], P('dp', 'tp'), parts along dimension 0
- output 6: bfloat16 [16384, 2048], P(('dp', 'tp')), parts along dimension 0
There are 4 independent parts. The reference program is written for one: setup_inputs(seed, part) draws one part's arguments, and reference() takes and returns one part's arrays. A program takes and returns all parts, laid end to end along the dimension named above; an argument that names none is the same for every part.
All inputs are finite; a program needn't handle non-finite values.
Results may differ from the reference program's by a relative error of at most 0.018.
Values are sent between devices in bfloat16 or wider.
A program may use at most 768 MiB of HBM per device.

```python
import jax
import jax.numpy as jnp
from jax import lax

ROWS = 2048
D = 2048
HEADS = 32
KV_HEADS = 16
HEAD = 128
THETA = 10000


def setup_inputs(seed: int = 0, part: int = 0) -> dict:
    kx, ky, kn, kq, kk, kv, ko = jax.random.split(jax.random.key(seed), 7)

    def weights(key, rows, columns):
        return jax.random.normal(key, (rows, columns), jnp.float32) * rows**-0.5

    drawn = {
        "x": jax.random.normal(jax.random.fold_in(kx, part), (ROWS, D), jnp.float32),
        "dy": jax.random.normal(jax.random.fold_in(ky, part), (ROWS, D), jnp.float32) * ROWS**-0.5,
        "gain": 1 + 0.1 * jax.random.normal(kn, (D,), jnp.float32),
        "wq": 2 * weights(kq, D, HEADS * HEAD),
        "wk": 2 * weights(kk, D, KV_HEADS * HEAD),
        "wv": 4 * weights(kv, D, KV_HEADS * HEAD),
        "wo": weights(ko, HEADS * HEAD, D),
    }
    return {k: v.astype(jnp.bfloat16) for k, v in drawn.items()}


def normed(x, gain):
    wide = x.astype(jnp.float32)
    scale = lax.rsqrt(jnp.mean(wide * wide, -1, keepdims=True) + 1e-6)
    return (wide * scale * gain.astype(jnp.float32)).astype(jnp.bfloat16)


def turned(t, place, theta):
    half = t.shape[-1] // 2
    angle = place.astype(jnp.float32)[:, None] * theta ** (-jnp.arange(half, dtype=jnp.float32) / half)
    cos, sin = jnp.cos(angle)[:, None], jnp.sin(angle)[:, None]
    a, b = t[..., :half].astype(jnp.float32), t[..., half:].astype(jnp.float32)
    return jnp.concatenate([a * cos - b * sin, b * cos + a * sin], -1).astype(jnp.bfloat16)


def matmul(a, w):
    return jnp.dot(a, w, preferred_element_type=jnp.float32).astype(jnp.bfloat16)


def einsum(form, a, b):
    return jnp.einsum(form, a.astype(jnp.float32), b.astype(jnp.float32))


def attention(q, k, v):
    scores = einsum("tgsd,ugd->gstu", q, k) * q.shape[-1] ** -0.5
    token = jnp.arange(q.shape[0])
    scores = jnp.where(token[:, None] >= token, scores, -jnp.inf)
    weights = jax.nn.softmax(scores, -1).astype(jnp.bfloat16)
    return einsum("gstu,ugd->tgsd", weights, v).astype(jnp.bfloat16)


def forward(x, gain, wq, wk, wv, wo):
    rows = x.shape[0]
    a, place = normed(x, gain), jnp.arange(rows)
    k = turned(matmul(a, wk).reshape(rows, -1, HEAD), place, THETA)
    q = turned(matmul(a, wq).reshape(rows, -1, HEAD), place, THETA).reshape(rows, k.shape[1], -1, HEAD)
    v = matmul(a, wv).reshape(rows, -1, HEAD)
    seen = attention(q, k, v).reshape(rows, -1)
    return (x.astype(jnp.float32) + jnp.dot(seen, wo, preferred_element_type=jnp.float32)).astype(jnp.bfloat16)


def reference(x, dy, gain, wq, wk, wv, wo):
    _, back = jax.vjp(forward, x, gain.astype(jnp.float32), wq, wk, wv, wo)
    by_x, by_gain, *by_weights = back(dy)
    return (by_x, by_gain[None], *by_weights)
```

```python
import functools

import jax
import jax.numpy as jnp
from jax import lax
from jax.experimental import pallas as pl
from jax.experimental.pallas import tpu as pltpu
from jax.sharding import PartitionSpec as P

HEAD = 128
THETA = 10000
LOG2E = 1.4426950408889634
HIDDEN = -2e30
F32, BF16 = jnp.float32, jnp.bfloat16


def _dot(a, b, ca, cb):
    return lax.dot_general(a, b, (((ca,), (cb,)), ((), ())), preferred_element_type=F32)


def _project(lo_ref, hi_ref, gain_ref, w_ref, cos_ref, sin_ref, a_ref, inv_ref, out_ref, *, turned):
    n = pl.program_id(0)
    half = lo_ref.shape[0]

    @pl.when(n == 0)
    def _():
        for at, ref in ((0, lo_ref), (half, hi_ref)):
            wide = ref[...].astype(F32)
            inv = lax.rsqrt(jnp.mean(wide * wide, -1, keepdims=True) + 1e-6)
            inv_ref[at : at + half, :] = inv
            a_ref[at : at + half, :] = (wide * inv * gain_ref[...].astype(F32)).astype(BF16)

    y = _dot(a_ref[...], w_ref[...], 1, 0).astype(BF16)

    @pl.when(n < turned)
    def _():
        cos, sin = cos_ref[...], sin_ref[...]
        for at in range(0, y.shape[1], HEAD):
            t = y[:, at : at + HEAD].astype(F32)
            out_ref[:, at : at + HEAD] = (t * cos + pltpu.roll(t, HEAD // 2, 1) * sin).astype(BF16)

    @pl.when(n >= turned)
    def _():
        out_ref[...] = y


def project(lo, hi, gain, w, cos, sin, turned_columns, block=512):
    rows, d = 2 * lo.shape[0], lo.shape[1]
    columns = w.shape[1]
    whole = lambda shape: pl.BlockSpec(shape, lambda n: (0, 0))
    return pl.pallas_call(
        functools.partial(_project, turned=turned_columns // block),
        grid=(columns // block,),
        in_specs=[whole(lo.shape), whole(hi.shape), whole((1, d)), pl.BlockSpec((d, block), lambda n: (0, n)), whole(cos.shape), whole(sin.shape)],
        out_specs=[whole((rows, d)), whole((rows, 1)), pl.BlockSpec((rows, block), lambda n: (0, n))],
        out_shape=[jax.ShapeDtypeStruct((rows, d), BF16), jax.ShapeDtypeStruct((rows, 1), F32), jax.ShapeDtypeStruct((rows, columns), BF16)],
        compiler_params=pltpu.CompilerParams(dimension_semantics=("arbitrary",), vmem_limit_bytes=32 * 2**20),
        cost_estimate=pl.CostEstimate(flops=2 * rows * d * columns, transcendentals=0, bytes_accessed=2 * (2 * rows * d + d * columns + rows * columns)),
        name="project",
    )(lo, hi, gain, w, cos, sin)


def _attend(pos_ref, q_ref, do_ref, *rest, slots, kb, first, last, scale):
    ks, vs, rest = rest[:slots], rest[slots : 2 * slots], rest[2 * slots :]
    cost_ref, sint_ref, rest = rest[0], rest[1], rest[2:]
    if last:
        cosk_ref, sink_ref, rest = rest[0], rest[1], rest[2:]
    if not first:
        dk_in, dv_in, rest = rest[0], rest[1], rest[2:]
    o_ref, dq_ref, dk_ref, dv_ref, kc, vc, qc, doc, s_s, o_s, dq_s, top_s, sum_s = rest[:13]
    dk_s, dv_s = rest[13:15] if last else (dk_ref, dv_ref)
    rows = q_ref.shape[0]
    g = q_ref.shape[1] // (kb * HEAD)
    half = rows // 2
    cols = g * rows
    e = scale * LOG2E
    mine = pos_ref[0]
    base = pl.multiple_of(mine * rows, rows)
    heads = range(kb)

    for s in range(slots):
        at = pl.ds(pl.multiple_of(pos_ref[1 + s] * rows, rows), rows)
        for i in heads:
            kc[i, at, :] = ks[s][:, i * HEAD : (i + 1) * HEAD]
            vc[i, at, :] = vs[s][:, i * HEAD : (i + 1) * HEAD]
    for i in heads:
        for n, (r, h) in enumerate((r, h) for r in range(2) for h in range(g)):
            here = slice(n * half, (n + 1) * half)
            there = slice((i * g + h) * HEAD, (i * g + h + 1) * HEAD)
            qc[i, here, :] = q_ref[r * half : (r + 1) * half, there]
            doc[i, here, :] = do_ref[r * half : (r + 1) * half, there]
    if first:
        dk_s[...] = jnp.zeros_like(dk_s)
        dv_s[...] = jnp.zeros_like(dv_s)
    else:
        dk_s[...] = dk_in[...]
        dv_s[...] = dv_in[...]

    wide = cols // 2
    gap = lax.rem(lax.broadcasted_iota(jnp.int32, (half, wide), 1), half) >= lax.broadcasted_iota(jnp.int32, (half, wide), 0)
    lane = lambda i: slice(i * HEAD, (i + 1) * HEAD)

    diagonal = ((pl.ds(base, half), 0), (pl.ds(pl.multiple_of(base + half, half), half), wide))

    for i in heads:
        parts = []
        for here, c in diagonal:
            s = _dot(kc[i, here, :], qc[i, c:, :], 1, 1)
            masked = jnp.where(gap, s[:, :wide], HIDDEN)
            s = masked if c else jnp.concatenate([masked, s[:, wide:]], 1)
            s_s[i, here, c:] = s
            parts.append((here, c, s))
        top = parts[0][2].max(0, keepdims=True)
        top = jnp.concatenate([top[:, :wide], jnp.maximum(top[:, wide:], parts[1][2].max(0, keepdims=True))], 1)
        top_s[i : i + 1, :] = top
        total, out = None, None
        for here, c, s in parts:
            p = jnp.exp2((s - top[:, c:]) * e)
            add, mix = p.sum(0, keepdims=True), _dot(vc[i, here, :].T, p.astype(BF16), 1, 0)
            if c:
                add = jnp.concatenate([total[:, :wide], total[:, wide:] + add], 1)
                mix = jnp.concatenate([out[:, :wide], out[:, wide:] + mix], 1)
            total, out = add, mix
        sum_s[i : i + 1, :] = total
        o_s[i] = out

    def forward(j, _):
        here = pl.ds(pl.multiple_of(j * rows, rows), rows)
        for i in heads:
            for c in (0, wide):
                cs = slice(c, c + wide)
                s = _dot(kc[i, here, :], qc[i, cs, :], 1, 1)
                s_s[i, here, cs] = s
                old = top_s[i : i + 1, cs]
                top = jnp.maximum(old, s.max(0, keepdims=True))
                keep = jnp.exp2((old - top) * e)
                p = jnp.exp2((s - top) * e)
                top_s[i : i + 1, cs] = top
                sum_s[i : i + 1, cs] = sum_s[i : i + 1, cs] * keep + p.sum(0, keepdims=True)
                o_s[i, :, cs] = o_s[i, :, cs] * keep + _dot(vc[i, here, :].T, p.astype(BF16), 1, 0)

    lax.fori_loop(0, mine, forward, None)

    lses, deltas = [], []
    for i in heads:
        total = sum_s[i : i + 1, :]
        out = (o_s[i] * (1 / total)).astype(BF16)
        deltas.append((out.astype(F32) * doc[i].astype(F32).T).sum(0, keepdims=True))
        lses.append(top_s[i : i + 1, :] * e + jnp.log2(total))
        flat = out.astype(F32).T.astype(BF16)
        for n, (r, h) in enumerate((r, h) for r in range(2) for h in range(g)):
            o_ref[r * half : (r + 1) * half, lane(i * g + h)] = flat[n * half : (n + 1) * half, :]

    def gradients(i, here, c0, c1):
        p = jnp.exp2(s_s[i, here, c0:c1] * e - lses[i][:, c0:c1])
        dp = _dot(vc[i, here, :], doc[i, c0:c1, :], 1, 1)
        ds = (p * (dp - deltas[i][:, c0:c1])).astype(BF16)
        return (_dot(p.astype(BF16), doc[i, c0:c1, :], 1, 0), _dot(ds, qc[i, c0:c1, :], 1, 0), _dot(kc[i, here, :].T, ds, 1, 0))

    for i in heads:
        for here, c in diagonal:
            dv, dk, dq = gradients(i, here, c, cols)
            dv_s[here, lane(i)] += dv
            dk_s[here, lane(i)] += dk
            if c:
                dq_s[i, :, c:] += dq
            else:
                dq_s[i] = dq

    def backward(j, _):
        here = pl.ds(pl.multiple_of(j * rows, rows), rows)
        for i in heads:
            dvs, dks = None, None
            for c in (0, wide):
                dv, dk, dq = gradients(i, here, c, c + wide)
                dq_s[i, :, c : c + wide] += dq
                dvs, dks = (dv, dk) if c == 0 else (dvs + dv, dks + dk)
            dv_s[here, lane(i)] += dvs
            dk_s[here, lane(i)] += dks

    lax.fori_loop(0, mine, backward, None)

    for i in heads:
        d = (dq_s[i] * scale).astype(BF16).astype(F32)
        a, b = d[: HEAD // 2], d[HEAD // 2 :]
        spread = lambda ref: jnp.concatenate([ref[:, r * half : (r + 1) * half] for r in range(2) for _ in range(g)], 1)
        cos, sin = spread(cost_ref), spread(sint_ref)
        flat = jnp.concatenate([a * cos + b * sin, b * cos - a * sin], 0).T.astype(BF16)
        for n, (r, h) in enumerate((r, h) for r in range(2) for h in range(g)):
            dq_ref[r * half : (r + 1) * half, lane(i * g + h)] = flat[n * half : (n + 1) * half, :]
    if last:
        for s in range(slots):
            at = pl.ds(pl.multiple_of(pos_ref[1 + s] * rows, rows), rows)
            to = slice(s * rows, (s + 1) * rows)
            dv_ref[to, :] = dv_s[at, :].astype(BF16)
            for i in heads:
                d = (dk_s[at, lane(i)] * scale).astype(BF16).astype(F32)
                dk_ref[to, lane(i)] = (d * cosk_ref[to, :] - pltpu.roll(d, HEAD // 2, 1) * sink_ref[to, :]).astype(BF16)


def attend_chunk(pos, q, do, ks, vs, cost, sint, cosk=None, sink=None, sums=None, *, last=False, kb=1, qat=0, kat=0, vat=0, kv_heads=4):
    rows, slots = do.shape[0], len(ks)
    qw = do.shape[1] // (kv_heads // kb)
    kw = kb * HEAD
    first = sums is None
    g = qw // kw
    cols = g * rows
    every = slots * rows
    fixed = lambda shape: pl.BlockSpec(shape, lambda h, _: (0, 0))
    column = lambda n, w, at=0: pl.BlockSpec((n, w), lambda h, _: (0, at + h))
    given = [q, do, *ks, *vs, cost, sint]
    specs = [column(rows, qw, qat), column(rows, qw)] + [column(rows, kw, kat)] * slots + [column(rows, kw, vat)] * slots + [fixed(cost.shape)] * 2
    if last:
        given += [cosk, sink]
        specs += [fixed(cosk.shape)] * 2
    alias = {}
    if not first:
        if not last:
            alias = {1 + len(given): 2, 2 + len(given): 3}
        given += list(sums)
        specs += [column(every, kw)] * 2
    kind = BF16 if last else F32
    width = kv_heads * HEAD
    scratch = [pltpu.VMEM((kb, every, HEAD), BF16)] * 2 + [pltpu.VMEM((kb, cols, HEAD), BF16)] * 2
    scratch += [pltpu.VMEM((kb, every, cols), F32)] + [pltpu.VMEM((kb, HEAD, cols), F32)] * 2 + [pltpu.VMEM((max(kb, 8), cols), F32)] * 2
    if last:
        scratch += [pltpu.VMEM((every, kw), F32)] * 2
    work = rows * every * do.shape[1] * 6
    return pl.pallas_call(
        functools.partial(_attend, slots=slots, kb=kb, first=first, last=last, scale=HEAD**-0.5),
        grid_spec=pltpu.PrefetchScalarGridSpec(
            num_scalar_prefetch=1,
            grid=(kv_heads // kb,),
            in_specs=specs,
            out_specs=[column(rows, qw), column(rows, qw), column(every, kw), column(every, kw)],
            scratch_shapes=scratch,
        ),
        out_shape=[jax.ShapeDtypeStruct(do.shape, BF16)] * 2 + [jax.ShapeDtypeStruct((every, width), kind)] * 2,
        input_output_aliases=alias,
        compiler_params=pltpu.CompilerParams(dimension_semantics=("arbitrary",), vmem_limit_bytes=(24 + 14 * kb) * 2**20),
        cost_estimate=pl.CostEstimate(flops=2 * work, transcendentals=0, bytes_accessed=2**24),
        name="attend",
    )(pos, *given)


def _normed_term(dq_ref, dk_ref, dv_ref, w_ref, x_lo, x_hi, inv_ref, lo_ref, hi_ref, g_ref, *, nq, nk):
    t = _dot(dq_ref[...], w_ref[:, :nq], 1, 1) + _dot(dk_ref[...], w_ref[:, nq : nq + nk], 1, 1) + _dot(dv_ref[...], w_ref[:, nq + nk :], 1, 1)
    half = lo_ref.shape[0]
    lo_ref[...] = t[:half].astype(BF16)
    hi_ref[...] = t[half:].astype(BF16)
    by_gain = (t[:half] * (x_lo[...].astype(F32) * inv_ref[:half])).sum(0, keepdims=True)
    by_gain += (t[half:] * (x_hi[...].astype(F32) * inv_ref[half:])).sum(0, keepdims=True)
    g_ref[...] = by_gain


def normed_term(dq, dk, dv, slot, w, lo, hi, inv, block=512):
    rows, nq, nk = dq.shape[0], dq.shape[1], dk.shape[1]
    d = w.shape[0]
    half = rows // 2
    column = lambda n: pl.BlockSpec((n, block), lambda i: (0, i))
    return pl.pallas_call(
        functools.partial(_normed_term, nq=nq, nk=nk),
        grid=(d // block,),
        in_specs=[pl.BlockSpec((rows, nq), lambda i: (0, 0)), pl.BlockSpec((rows, nk), lambda i: (slot, 0)), pl.BlockSpec((rows, nk), lambda i: (slot, 0)),
                  pl.BlockSpec((block, w.shape[1]), lambda i: (i, 0)), column(half), column(half), pl.BlockSpec((rows, 1), lambda i: (0, 0))],
        out_specs=[column(half), column(half), column(1)],
        out_shape=[jax.ShapeDtypeStruct((half, d), BF16)] * 2 + [jax.ShapeDtypeStruct((1, d), F32)],
        compiler_params=pltpu.CompilerParams(dimension_semantics=("arbitrary",), vmem_limit_bytes=32 * 2**20),
        cost_estimate=pl.CostEstimate(flops=2 * rows * d * w.shape[1], transcendentals=0, bytes_accessed=2 * (rows * w.shape[1] + d * w.shape[1] + 2 * rows * d)),
        name="normed_term",
    )(dq, dk, dv, w, lo, hi, inv)


def solution(mesh):
    size = mesh.shape["tp"]
    to_right = [(i, (i + 1) % size) for i in range(size)]
    to_left = [(i, (i - 1) % size) for i in range(size)]

    def right(t):
        return lax.ppermute(t, "tp", to_right)

    def left(t):
        return lax.ppermute(t, "tp", to_left)

    def gather(lo, hi):
        l_lo, r_hi = right(lo), left(hi)
        l_hi, r_lo = right(hi), left(lo)
        o_lo, o_hi = right(l_lo), left(r_hi)
        return [(lo, hi), (l_lo, l_hi), (r_lo, r_hi), (o_lo, o_hi)]

    def step(x, dy, gain, wq, wk, wv, wo):
        rows, half = x.shape[0], x.shape[0] // 2
        me = lax.axis_index("tp")
        order = jnp.stack([me, (me + size - 1) % size, (me + 1) % size, (me + 2) % size]).astype(jnp.int32)
        xs = gather(x[:half], x[half:])
        dy_lo, dy_hi = dy[:half], dy[half:]
        dy_lo, dy_hi, _ = lax.optimization_barrier((dy_lo, dy_hi, xs[1][0]))
        dys = gather(dy_lo, dy_hi)

        place = (order[:, None] * rows + jnp.arange(rows, dtype=jnp.int32)[None]).reshape(-1).astype(jnp.float32)
        n = HEAD // 2
        angle = place[:, None] * THETA ** (-jnp.arange(n, dtype=F32) / n)
        cos, sin = jnp.cos(angle), jnp.sin(angle)
        cos2, sin2 = jnp.concatenate([cos, cos], 1), jnp.concatenate([-sin, sin], 1)
        cost, sint = cos.T, sin.T

        w = jnp.concatenate([wq, wk, wv], 1)
        nq, nk = wq.shape[1], wk.shape[1]
        kv_heads = nk // HEAD
        flat = gain[None]
        a, inv, qkv = [], [], []
        for s in range(size):
            at = slice(s * rows, (s + 1) * rows)
            got = project(*xs[s], flat, w, cos2[at], sin2[at], nq + nk)
            a.append(got[0]), inv.append(got[1]), qkv.append(got[2])

        kb = 1
        sums = None
        seen, dqs = [], []
        dchunks = [jnp.concatenate(d, 0) for d in dys]
        for s in range(size):
            at = slice(s * rows, (s + 1) * rows)
            do = _dot(dchunks[s], wo, 1, 1).astype(BF16)
            pos = jnp.concatenate([order[s : s + 1], order])
            last = s == size - 1
            o, dq, dk, dv = attend_chunk(pos, qkv[s], do, qkv, qkv, cost[:, at], sint[:, at], cos2 if last else None, sin2 if last else None, sums,
                                         last=last, kb=kb, qat=0, kat=nq // (kb * HEAD), vat=(nq + nk) // (kb * HEAD), kv_heads=kv_heads)
            sums = (dk, dv)
            seen.append(o), dqs.append(dq)

        terms = {}
        for s in (3, 2, 1, 0):
            terms[s] = normed_term(dqs[s], dk, dv, s, w, *xs[s], inv[s])
        o_lo, o_hi = right(terms[3][0]), left(terms[3][1])
        from_l_hi, from_r_lo = right(terms[2][1]), left(terms[1][0])
        add = lambda t, got: (t.astype(F32) + got.astype(F32)).astype(BF16)
        from_l_lo, from_r_hi = right(add(terms[2][0], o_lo)), left(add(terms[1][1], o_hi))
        by_gain = lax.psum(terms[0][2] + terms[1][2] + terms[2][2] + terms[3][2], "tp")

        every_a, every_dy = jnp.concatenate(a, 0), jnp.concatenate(dchunks, 0)
        by_wo = _dot(jnp.concatenate(seen, 0), every_dy, 0, 0).astype(BF16)
        every_dq = jnp.concatenate(dqs, 0)
        by_wq = _dot(every_a, every_dq, 0, 0).astype(BF16)
        by_wk = _dot(every_a, dk, 0, 0).astype(BF16)
        by_wv = _dot(every_a, dv, 0, 0).astype(BF16)

        def finish(part, own, one, two, inv, dy):
            wide, hat_gain = part.astype(F32), gain.astype(F32)
            t = (own.astype(F32) + one.astype(F32) + two.astype(F32)) * hat_gain
            hat = wide * inv
            return (dy.astype(F32) + inv * (t - hat * jnp.mean(t * hat, -1, keepdims=True))).astype(BF16)

        by_x = jnp.concatenate([
            finish(x[:half], terms[0][0], from_l_lo, from_r_lo, inv[0][:half], dy[:half]),
            finish(x[half:], terms[0][1], from_l_hi, from_r_hi, inv[0][half:], dy[half:]),
        ], 0)
        return by_x, by_gain, by_wq, by_wk, by_wv, by_wo

    tokens, columns = P(("dp", "tp"), None), P(None, "tp")
    return jax.shard_map(
        step,
        mesh=mesh,
        in_specs=(tokens, tokens, P(None), columns, columns, columns, P("tp", None)),
        out_specs=(tokens, P("dp", None), P("dp", "tp"), P("dp", "tp"), P("dp", "tp"), P(("dp", "tp"), None)),
        check_vma=False,
    )
```

```python
import functools

import jax
import jax.numpy as jnp
import numpy as np
from jax import lax
from jax.experimental import pallas as pl
from jax.experimental.pallas import tpu as pltpu
from jax.sharding import PartitionSpec as P

HEAD = 128
THETA = 10000
LOG2E = 1.4426950408889634
HIDDEN = -2e30
F32, BF16 = jnp.float32, jnp.bfloat16


def _dot(a, b, ca, cb):
    return lax.dot_general(a, b, (((ca,), (cb,)), ((), ())), preferred_element_type=F32)


OFFSETS = (0, 0, 3, 1, 3, 1, 2, 2)
HALVES = (0, 1, 0, 1, 1, 0, 0, 1)
MESH = pl.DeviceIdType.MESH


def _place(me, u, size):
    group, b = lax.div(u, 2), lax.rem(u, 2)
    middle = lax.rem(lax.div(group + 1, 2), 2)
    end = lax.div(group, 3)
    swapped = lax.div(group, 2) * (1 - end)
    off = middle * (3 - 2 * b) + end * 2
    half = b + swapped * (1 - 2 * b)
    return lax.rem(me + off, size) * 2 + half


def _lanes(h, width):
    return pl.ds(pl.multiple_of(h * width, width), width)


def _attention(x_ref, dy_ref, gain_ref, wq_ref, wk_ref, wv_ref, wo_ref, cs_ref,
               x_all, dy_all, a_all, inv_all, o_all, dq_all, dk_all, dv_all,
               dyb, qc, kc, vc, kt, vt, wo_s, xb, ab, doc, o_st, dq_st, acc_o, acc_dq, top_s, lse_s,
               x_send, x_recv, dy_send, dy_recv, w_sem, load_sem, out_sem, *, size, g, scale):
    unit, d = xb.shape
    kv = kc.shape[0]
    units = 2 * size
    kb = 2
    cols = g * unit
    e = scale * LOG2E
    me = lax.axis_index("tp")
    right = {"tp": lax.rem(me + 1, size)}
    left = {"tp": lax.rem(me + size - 1, size)}

    barrier = pltpu.get_barrier_semaphore()
    for other in (left, right):
        pl.semaphore_signal(barrier, inc=1, device_id=other, device_id_type=MESH)
    pl.semaphore_wait(barrier, 2)

    def half(ref, n):
        return ref.at[pl.ds(n * unit, unit), :]

    def remote(source, target, send, recv, u, other):
        return pltpu.make_async_remote_copy(src_ref=source, dst_ref=target.at[u], send_sem=send.at[u], recv_sem=recv.at[u], device_id=other, device_id_type=MESH)

    def own_copies(ref, target, send, recv, stage):
        n = 2 + 2 * stage
        return (remote(half(ref, stage), target, send, recv, n, right), remote(half(ref, 1 - stage), target, send, recv, n + 1, left))

    def passed_on(target, send, recv):
        return (remote(target.at[2], target, send, recv, 6, right), remote(target.at[3], target, send, recv, 7, left))

    def start(copies):
        for c in copies:
            c.start()

    for stage in (0, 1):
        start(own_copies(x_ref, x_all, x_send, x_recv, stage))
    dy_loads = [pltpu.make_async_copy(half(dy_ref, n), dyb.at[n], w_sem.at[4 + n]) for n in range(2)]
    wo_load = pltpu.make_async_copy(wo_ref, wo_s, w_sem.at[3])

    def arrived(target, send, recv, u):
        remote(target.at[2], target, send, recv, u, right).wait_recv()

    def rotation(at):
        t = cs_ref[pl.ds(at, unit), :]
        low = lax.broadcasted_iota(jnp.int32, t.shape, 1) < HEAD // 2
        turned = pltpu.roll(t, HEAD // 2, 1)
        return jnp.where(low, t, turned), jnp.where(low, -turned, t)

    def project(w_s):
        loads, at = [], 0
        for n, ref in enumerate((wq_ref, wk_ref, wv_ref)):
            loads.append(pltpu.make_async_copy(ref, w_s.at[:, pl.ds(at, ref.shape[1])], w_sem.at[n]))
            at += ref.shape[1]
        start(loads)
        start(dy_loads)
        wo_load.start()
        block = kv * HEAD

        def one(u, _):
            @pl.when(u == 2)
            def _():
                arrived(x_all, x_send, x_recv, 2)
                arrived(x_all, x_send, x_recv, 3)
                start(passed_on(x_all, x_send, x_recv))
                start(own_copies(dy_ref, dyb, dy_send, dy_recv, 0))

            @pl.when(u >= 4)
            def _():
                arrived(x_all, x_send, x_recv, u)

            @pl.when(u == 4)
            def _():
                start(own_copies(dy_ref, dyb, dy_send, dy_recv, 1))

            @pl.when(u < 2)
            def _():
                c = pltpu.make_async_copy(x_ref.at[pl.ds(pl.multiple_of(u * unit, unit), unit), :], xb, load_sem)
                c.start()
                c.wait()

            @pl.when(u >= 2)
            def _():
                c = pltpu.make_async_copy(x_all.at[u], xb, load_sem)
                c.start()
                c.wait()

            @pl.when(u >= 1)
            def _():
                pltpu.make_async_copy(ab, a_all.at[u - 1], out_sem.at[0]).wait()

            wide = xb[...].astype(F32)
            inv = lax.rsqrt(jnp.mean(wide * wide, -1, keepdims=True) + 1e-6)
            rows = pl.ds(pl.multiple_of(u * unit, unit), unit)
            inv_all[rows, :] = inv
            ab[...] = (wide * inv * gain_ref[...].astype(F32)).astype(BF16)
            pltpu.make_async_copy(ab, a_all.at[u], out_sem.at[0]).start()

            @pl.when(u == 0)
            def _():
                for c in loads:
                    c.wait()

            at = pl.multiple_of(_place(me, u, size) * unit, unit)
            here = pl.ds(at, unit)
            cos, sin = rotation(at)
            for n in range(g + 2):
                y = _dot(ab[...], w_s[:, n * block : (n + 1) * block], 1, 0).astype(BF16)
                for h in range(kv):
                    t = y[:, h * HEAD : (h + 1) * HEAD]
                    if n < g + 1:
                        t = t.astype(F32)
                        t = (t * cos + pltpu.roll(t, HEAD // 2, 1) * sin).astype(BF16)
                    if n < g:
                        head = n * kv + h
                        qc[u, head // g, (head % g) * unit : (head % g + 1) * unit, :] = t
                    else:
                        (kc if n == g else vc)[h, here, :] = t
                        (kt if n == g else vt)[h, :, here] = t.T

        lax.fori_loop(0, units, one, None)
        pltpu.make_async_copy(ab, a_all.at[units - 1], out_sem.at[0]).wait()
        for stage in (0, 1):
            for c in own_copies(x_ref, x_all, x_send, x_recv, stage):
                c.wait_send()
        for c in passed_on(x_all, x_send, x_recv):
            c.wait_send()

    pl.run_scoped(project, pltpu.VMEM((d, (g + 2) * kv * HEAD), BF16))
    for c in dy_loads:
        c.wait()
    wo_load.wait()

    def attend(s_s, dk_s, dv_s):
        dk_s[...] = jnp.zeros_like(dk_s)
        dv_s[...] = jnp.zeros_like(dv_s)
        big = 2 * unit

        def one(u, _):
            @pl.when(u == 2)
            def _():
                arrived(dyb, dy_send, dy_recv, 2)
                arrived(dyb, dy_send, dy_recv, 3)
                start(passed_on(dyb, dy_send, dy_recv))

            @pl.when(u >= 4)
            def _():
                arrived(dyb, dy_send, dy_recv, u)

            pltpu.make_async_copy(dyb.at[u], dy_all.at[u], out_sem.at[3]).start()
            block = 4 * HEAD
            for n in range(g * kv // 4):
                y = _dot(dyb[u], wo_s[n * block : (n + 1) * block, :], 1, 1).astype(BF16)
                for h in range(4):
                    head = n * 4 + h
                    doc[head // g, (head % g) * unit : (head % g + 1) * unit, :] = y[:, h * HEAD : (h + 1) * HEAD]

            place = _place(me, u, size)
            at = pl.multiple_of(place * unit, unit)
            whole = lax.div(place, 2)
            odd = lax.rem(place, 2)

            @pl.when(u >= 1)
            def _():
                pltpu.make_async_copy(o_st, o_all.at[u - 1], out_sem.at[1]).wait()
                pltpu.make_async_copy(dq_st, dq_all.at[u - 1], out_sem.at[2]).wait()

            def pair(hp, _):
                heads = [(i, hp * kb + i) for i in range(kb)]

                def score(here, gap=None):
                    for i, h in heads:
                        s = _dot(kc[h, here, :], qc[u, h], 1, 1) * e
                        if gap is not None:
                            ok = lax.rem(lax.broadcasted_iota(jnp.int32, s.shape, 1), unit) + gap >= lax.broadcasted_iota(jnp.int32, s.shape, 0)
                            s = jnp.where(ok, s, HIDDEN)
                        s_s[i, here, :] = s
                        top_s[i : i + 1, :] = jnp.maximum(top_s[i : i + 1, :], s.max(0, keepdims=True))

                def mix(here):
                    for i, h in heads:
                        p = jnp.exp2(s_s[i, here, :] - top_s[i : i + 1, :])
                        lse_s[i : i + 1, :] += p.sum(0, keepdims=True)
                        acc_o[i] += _dot(vt[h, :, here], p.astype(BF16), 1, 0)

                def gradients(here, lses, deltas):
                    for i, h in heads:
                        p = jnp.exp2(s_s[i, here, :] - lses[i])
                        dp = _dot(vc[h, here, :], doc[h], 1, 1)
                        ds = (p * (dp - deltas[i])).astype(BF16)
                        dv_s[h, here, :] += _dot(p.astype(BF16), doc[h], 1, 0)
                        dk_s[h, here, :] += _dot(ds, qc[u, h], 1, 0)
                        acc_dq[i] += _dot(kt[h, :, here], ds, 1, 0)

                small = lambda j: pl.ds(pl.multiple_of(at - j * unit, unit), unit)
                large = lambda j: pl.ds(pl.multiple_of(j * big, big), big)
                top_s[...] = jnp.full_like(top_s, HIDDEN)
                lse_s[...] = jnp.zeros_like(lse_s)
                acc_o[...] = jnp.zeros_like(acc_o)
                acc_dq[...] = jnp.zeros_like(acc_dq)
                lax.fori_loop(0, whole, lambda j, _: score(large(j)), None)
                lax.fori_loop(0, odd + 1, lambda j, _: score(small(j), j * unit), None)
                lax.fori_loop(0, whole, lambda j, _: mix(large(j)), None)
                lax.fori_loop(0, odd + 1, lambda j, _: mix(small(j)), None)
                for i, h in heads:
                    total = lse_s[i : i + 1, :]
                    out = (acc_o[i] * (1 / total)).astype(BF16).astype(F32)
                    lse_s[i : i + 1, :] = top_s[i : i + 1, :] + jnp.log2(total)
                    top_s[i : i + 1, :] = (out * doc[h].astype(F32).T).sum(0, keepdims=True)
                    flat = out.T.astype(BF16)
                    for n in range(g):
                        o_st[:, _lanes(h * g + n, HEAD)] = flat[n * unit : (n + 1) * unit, :]
                lses = [lse_s[i : i + 1, :] for i in range(kb)]
                deltas = [top_s[i : i + 1, :] for i in range(kb)]
                lax.fori_loop(0, whole, lambda j, _: gradients(large(j), lses, deltas), None)
                lax.fori_loop(0, odd + 1, lambda j, _: gradients(small(j), lses, deltas), None)
                t = cs_ref[pl.ds(at, unit), :].T
                cos, sin = (jnp.concatenate([v] * g, 1) for v in (t[: HEAD // 2], t[HEAD // 2 :]))
                for i, h in heads:
                    dq = (acc_dq[i] * scale).astype(BF16).astype(F32)
                    a, b = dq[: HEAD // 2], dq[HEAD // 2 :]
                    flat = jnp.concatenate([a * cos + b * sin, b * cos - a * sin], 0).T.astype(BF16)
                    for n in range(g):
                        dq_st[:, _lanes(h * g + n, HEAD)] = flat[n * unit : (n + 1) * unit, :]

            lax.fori_loop(0, kv // kb, pair, None)
            pltpu.make_async_copy(o_st, o_all.at[u], out_sem.at[1]).start()
            pltpu.make_async_copy(dq_st, dq_all.at[u], out_sem.at[2]).start()
            pltpu.make_async_copy(dyb.at[u], dy_all.at[u], out_sem.at[3]).wait()

        lax.fori_loop(0, units, one, None)

        def last(u, _):
            at = pl.multiple_of(_place(me, u, size) * unit, unit)
            cos, sin = rotation(at)
            rows = pl.ds(pl.multiple_of(u * unit, unit), unit)
            for h in range(kv):
                dv_all[rows, h * HEAD : (h + 1) * HEAD] = dv_s[h, pl.ds(at, unit), :].astype(BF16)
                t = (dk_s[h, pl.ds(at, unit), :] * scale).astype(BF16).astype(F32)
                dk_all[rows, h * HEAD : (h + 1) * HEAD] = (t * cos - pltpu.roll(t, HEAD // 2, 1) * sin).astype(BF16)

        lax.fori_loop(0, units, last, None)

    every = units * unit
    pl.run_scoped(attend, pltpu.VMEM((kb, every, cols), F32), pltpu.VMEM((kv, every, HEAD), F32), pltpu.VMEM((kv, every, HEAD), F32))
    pltpu.make_async_copy(o_st, o_all.at[units - 1], out_sem.at[1]).wait()
    pltpu.make_async_copy(dq_st, dq_all.at[units - 1], out_sem.at[2]).wait()
    for stage in (0, 1):
        for c in own_copies(dy_ref, dyb, dy_send, dy_recv, stage):
            c.wait_send()
    for c in passed_on(dyb, dy_send, dy_recv):
        c.wait_send()


def attention(x, dy, gain, wq, wk, wv, wo, cs, size):
    rows, d = x.shape
    unit, units = rows // 2, 2 * size
    nq, nk = wq.shape[1], wk.shape[1]
    kv, g = nk // HEAD, nq // nk
    every, cols = units * unit, g * unit
    anywhere, vmem = pl.BlockSpec(memory_space=pl.ANY), pl.BlockSpec(memory_space=pltpu.VMEM)
    in_hbm = lambda n: jax.ShapeDtypeStruct((units, unit, n), BF16)
    dma = pltpu.SemaphoreType.DMA
    return pl.pallas_call(
        functools.partial(_attention, size=size, g=g, scale=HEAD**-0.5),
        in_specs=[anywhere, anywhere, vmem, anywhere, anywhere, anywhere, anywhere, vmem],
        out_specs=[anywhere, anywhere, anywhere, vmem, anywhere, anywhere, vmem, vmem],
        out_shape=[in_hbm(d), in_hbm(d), in_hbm(d), jax.ShapeDtypeStruct((every, 1), F32), in_hbm(nq), in_hbm(nq),
                   jax.ShapeDtypeStruct((every, nk), BF16), jax.ShapeDtypeStruct((every, nk), BF16)],
        scratch_shapes=[
            pltpu.VMEM((units, unit, d), BF16), pltpu.VMEM((units, kv, cols, HEAD), BF16),
            pltpu.VMEM((kv, every, HEAD), BF16), pltpu.VMEM((kv, every, HEAD), BF16),
            pltpu.VMEM((kv, HEAD, every), BF16), pltpu.VMEM((kv, HEAD, every), BF16),
            pltpu.VMEM((nq, d), BF16), pltpu.VMEM((unit, d), BF16), pltpu.VMEM((unit, d), BF16),
            pltpu.VMEM((kv, cols, HEAD), BF16), pltpu.VMEM((unit, nq), BF16), pltpu.VMEM((unit, nq), BF16),
            pltpu.VMEM((2, HEAD, cols), F32), pltpu.VMEM((2, HEAD, cols), F32), pltpu.VMEM((8, cols), F32), pltpu.VMEM((8, cols), F32),
            dma((units,)), dma((units,)), dma((units,)), dma((units,)), dma((6,)), dma, dma((4,)),
        ],
        compiler_params=pltpu.CompilerParams(collective_id=0, has_side_effects=True, vmem_limit_bytes=61 * 2**20),
        cost_estimate=pl.CostEstimate(flops=10**11, transcendentals=0, bytes_accessed=2**26),
        name="attention",
    )(x, dy, gain, wq, wk, wv, wo, cs)


def _normed_term(dq_ref, dk_ref, dv_ref, wq_ref, wk_ref, wv_ref, x_ref, inv_ref, lo_ref, hi_ref, g_ref):
    unit = lo_ref.shape[0]
    dq = dq_ref[...].reshape(2 * unit, -1)
    t = _dot(dq, wq_ref[...], 1, 1) + _dot(dk_ref[...], wk_ref[...], 1, 1) + _dot(dv_ref[...], wv_ref[...], 1, 1)
    lo_ref[...] = t[:unit].astype(BF16)
    hi_ref[...] = t[unit:].astype(BF16)
    g_ref[...] = (t * (x_ref[...].reshape(t.shape).astype(F32) * inv_ref[...])).sum(0, keepdims=True)


def normed_term(dq, dk, dv, units, wq, wk, wv, x, inv, block=512):
    unit, nq, nk = dq.shape[1], wq.shape[1], wk.shape[1]
    d = wq.shape[0]
    n = units[0] // 2
    x = x.reshape(-1, unit, d)
    pair = lambda w: pl.BlockSpec((2 * unit, w), lambda i: (n, 0))
    row = lambda w: pl.BlockSpec((block, w), lambda i: (i, 0))
    column = lambda r: pl.BlockSpec((r, block), lambda i: (0, i))
    return pl.pallas_call(
        _normed_term,
        grid=(d // block,),
        in_specs=[pl.BlockSpec((2, unit, nq), lambda i: (n, 0, 0)), pair(nk), pair(nk), row(nq), row(nk), row(nk),
                  pl.BlockSpec((2, unit, block), lambda i: (n, 0, i)), pair(1)],
        out_specs=[column(unit), column(unit), column(1)],
        out_shape=[jax.ShapeDtypeStruct((unit, d), BF16)] * 2 + [jax.ShapeDtypeStruct((1, d), F32)],
        compiler_params=pltpu.CompilerParams(dimension_semantics=("arbitrary",), vmem_limit_bytes=32 * 2**20),
        cost_estimate=pl.CostEstimate(flops=4 * unit * d * (nq + 2 * nk), transcendentals=0, bytes_accessed=2 * (2 * unit + d) * (nq + 2 * nk) + 8 * unit * d),
        name="normed_term",
    )(dq, dk, dv, wq, wk, wv, x, inv)


def angles(rows):
    n = HEAD // 2
    angle = np.arange(rows, dtype=np.float32)[:, None] * np.float32(THETA) ** (-np.arange(n, dtype=np.float32) / np.float32(n))
    angle = angle.astype(np.float64)
    return np.concatenate([np.cos(angle), np.sin(angle)], 1).astype(np.float32)


def solution(mesh):
    size = mesh.shape["tp"]
    to_right = [(i, (i + 1) % size) for i in range(size)]
    to_left = [(i, (i - 1) % size) for i in range(size)]

    def right(t):
        return lax.ppermute(t, "tp", to_right)

    def left(t):
        return lax.ppermute(t, "tp", to_left)

    def step(x, dy, gain, wq, wk, wv, wo):
        rows, d = x.shape
        half = rows // 2
        x_all, dy_all, a_all, inv, o_all, dq, dk, dv = attention(x, dy, gain[None], wq, wk, wv, wo, jnp.asarray(angles(size * rows)), size)

        def term(units):
            return normed_term(dq, dk, dv, units, wq, wk, wv, x if units[0] < 2 else x_all, inv)

        add = lambda t, got: (t.astype(F32) + got.astype(F32)).astype(BF16)
        opp_lo, opp_hi, g3 = term((6, 7))
        o_lo, o_hi = right(opp_lo), left(opp_hi)
        lf_lo, rt_hi, g1 = term((2, 3))
        from_l_hi, from_r_lo = right(rt_hi), left(lf_lo)
        lf_hi, rt_lo, g2 = term((4, 5))
        from_l_lo, from_r_hi = right(add(rt_lo, o_lo)), left(add(lf_hi, o_hi))
        own_lo, own_hi, g0 = term((0, 1))
        by_gain = lax.psum(g0 + g1 + g2 + g3, "tp")

        flat = lambda t: t.reshape(-1, t.shape[-1])
        by_wo = _dot(flat(o_all), flat(dy_all), 0, 0).astype(BF16)
        a_all = flat(a_all)
        by_wq = _dot(a_all, flat(dq), 0, 0).astype(BF16)
        by_wk = _dot(a_all, dk, 0, 0).astype(BF16)
        by_wv = _dot(a_all, dv, 0, 0).astype(BF16)

        wide, inv = x.astype(F32), inv[:rows]
        t = jnp.concatenate([
            own_lo.astype(F32) + from_l_lo.astype(F32) + from_r_lo.astype(F32),
            own_hi.astype(F32) + from_l_hi.astype(F32) + from_r_hi.astype(F32)]) * gain.astype(F32)
        hat = wide * inv
        by_x = (dy.astype(F32) + inv * (t - hat * jnp.mean(t * hat, -1, keepdims=True))).astype(BF16)
        return by_x, by_gain, by_wq, by_wk, by_wv, by_wo

    tokens, columns = P(("dp", "tp"), None), P(None, "tp")
    return jax.shard_map(
        step,
        mesh=mesh,
        in_specs=(tokens, tokens, P(None), columns, columns, columns, P("tp", None)),
        out_specs=(tokens, P("dp", None), P("dp", "tp"), P("dp", "tp"), P("dp", "tp"), P(("dp", "tp"), None)),
        check_vma=False,
    )
```

```python
import functools

import jax
import jax.numpy as jnp
import numpy as np
from jax import lax
from jax.experimental import pallas as pl
from jax.experimental.pallas import tpu as pltpu
from jax.sharding import PartitionSpec as P


HEAD = 128
THETA = 10000
LOG2E = 1.4426950408889634
NEG = -1e30
HIDDEN = -2e30
F32, BF16 = jnp.float32, jnp.bfloat16


def _dot(a, b, ca, cb):
    return lax.dot_general(a, b, (((ca,), (cb,)), ((), ())), preferred_element_type=F32)


MESH = pl.DeviceIdType.MESH


def _place(me, u, size):
    group, b = lax.div(u, 2), lax.rem(u, 2)
    middle = lax.rem(lax.div(group + 1, 2), 2)
    end = lax.div(group, 3)
    swapped = lax.div(group, 2) * (1 - end)
    off = middle * (3 - 2 * b) + end * 2
    half = b + swapped * (1 - 2 * b)
    return lax.rem(me + off, size) * 2 + half


def _lanes(h, width):
    return pl.ds(pl.multiple_of(h * width, width), width)


def _attention(x_ref, dy_ref, gain_ref, wq_ref, wk_ref, wv_ref, wo_ref, cs_ref,
               x_all, dy_all, a_all, inv_all, o_all, dq_all, dk_all, dv_all,
               dyb, qc, kc, vc, kt, vt, wo_s, xb, ab, doc, o_st, dq_st, acc_o, acc_dq, top_s, sum_s, row_s,
               x_send, x_recv, dy_send, dy_recv, w_sem, load_sem, out_sem, *, size, g, scale):
    unit, d = ab.shape
    kv = kc.shape[0]
    units = 2 * size
    kb = 2
    cols = g * unit
    e = scale * LOG2E
    me = lax.axis_index("tp")
    right = {"tp": lax.rem(me + 1, size)}
    left = {"tp": lax.rem(me + size - 1, size)}

    barrier = pltpu.get_barrier_semaphore()
    for other in (left, right):
        pl.semaphore_signal(barrier, inc=1, device_id=other, device_id_type=MESH)
    pl.semaphore_wait(barrier, 2)

    def half(ref, n):
        return ref.at[pl.ds(n * unit, unit), :]

    def remote(source, target, send, recv, u, other):
        return pltpu.make_async_remote_copy(src_ref=source, dst_ref=target.at[u], send_sem=send.at[u], recv_sem=recv.at[u], device_id=other, device_id_type=MESH)

    def own_copies(ref, target, send, recv, stage):
        n = 2 + 2 * stage
        return (remote(half(ref, stage), target, send, recv, n, right), remote(half(ref, 1 - stage), target, send, recv, n + 1, left))

    def passed_on(target, send, recv):
        return (remote(target.at[2], target, send, recv, 6, right), remote(target.at[3], target, send, recv, 7, left))

    def start(copies):
        for c in copies:
            c.start()

    for stage in (0, 1):
        start(own_copies(x_ref, x_all, x_send, x_recv, stage))
    dy_loads = [pltpu.make_async_copy(half(dy_ref, n), dyb.at[n], w_sem.at[4 + n]) for n in range(2)]
    wo_load = pltpu.make_async_copy(wo_ref, wo_s, w_sem.at[3])

    def arrived(target, send, recv, u):
        remote(target.at[2], target, send, recv, u, right).wait_recv()

    def rotation(at):
        t = cs_ref[pl.ds(at, unit), :]
        low = lax.broadcasted_iota(jnp.int32, t.shape, 1) < HEAD // 2
        turned = pltpu.roll(t, HEAD // 2, 1)
        return jnp.where(low, t, turned), jnp.where(low, -turned, t)

    big = 2 * unit
    top_s[...] = jnp.full_like(top_s, NEG)
    sum_s[...] = jnp.zeros_like(sum_s)
    acc_o[...] = jnp.zeros_like(acc_o)

    def mask(shape, gap):
        return lax.rem(lax.broadcasted_iota(jnp.int32, shape, 1), unit) + gap >= lax.broadcasted_iota(jnp.int32, shape, 0)

    def project(w_s, s_s):
        loads, at = [], 0
        for n, ref in enumerate((wq_ref, wk_ref, wv_ref)):
            loads.append(pltpu.make_async_copy(ref, w_s.at[:, pl.ds(at, ref.shape[1])], w_sem.at[n]))
            at += ref.shape[1]
        start(loads)
        start(dy_loads)
        wo_load.start()
        block = kv * HEAD

        def forward(row, at, n, gap=None):
            here = pl.ds(pl.multiple_of(at, n), n)
            tops = {}
            for h in range(kv + 1):
                if h < kv:
                    s = _dot(kc[h, here, :], qc[row, h], 1, 1) * e
                    if gap is not None:
                        s = jnp.where(mask(s.shape, gap), s, HIDDEN)
                    s_s[h, :n, :] = s
                    old = top_s[row, h : h + 1, :]
                    tops[h] = old, jnp.maximum(old, s.max(0, keepdims=True))
                    top_s[row, h : h + 1, :] = tops[h][1]
                if h:
                    i = h - 1
                    old, top = tops[i]
                    keep = jnp.exp2(old - top)
                    p = jnp.exp2(s_s[i, :n, :] - top)
                    sum_s[row, i : i + 1, :] = sum_s[row, i : i + 1, :] * keep + p.sum(0, keepdims=True)
                    acc_o[row, i] = acc_o[row, i] * keep + _dot(vt[i, :, here], p.astype(BF16), 1, 0)

        def one(u, _):
            @pl.when(lax.rem(u, 2) == 0)
            def _():
                @pl.when(u >= 2)
                def _():
                    arrived(x_all, x_send, x_recv, u)
                    arrived(x_all, x_send, x_recv, u + 1)
                    for n in range(2):
                        pltpu.make_async_copy(x_all.at[u + n], xb.at[n], load_sem.at[n]).start()

                @pl.when(u < 2)
                def _():
                    for n in range(2):
                        pltpu.make_async_copy(half(x_ref, n), xb.at[n], load_sem.at[n]).start()

            @pl.when(u == 2)
            def _():
                start(passed_on(x_all, x_send, x_recv))
                start(own_copies(dy_ref, dyb, dy_send, dy_recv, 0))

            @pl.when(u == 4)
            def _():
                start(own_copies(dy_ref, dyb, dy_send, dy_recv, 1))

            now = lax.rem(u, 2)
            pltpu.make_async_copy(x_all.at[u], xb.at[now], load_sem.at[now]).wait()

            @pl.when(u < 2)
            def _():
                c = pltpu.make_async_copy(xb.at[now], x_all.at[u], out_sem.at[4])
                c.start()
                c.wait()

            @pl.when(u >= 1)
            def _():
                pltpu.make_async_copy(ab, a_all.at[u - 1], out_sem.at[0]).wait()

            wide = xb[now].astype(F32)
            inv = lax.rsqrt(jnp.mean(wide * wide, -1, keepdims=True) + 1e-6)
            rows = pl.ds(pl.multiple_of(u * unit, unit), unit)
            inv_all[rows, :] = inv
            ab[...] = (wide * inv * gain_ref[...].astype(F32)).astype(BF16)
            pltpu.make_async_copy(ab, a_all.at[u], out_sem.at[0]).start()

            @pl.when(u == 0)
            def _():
                for c in loads:
                    c.wait()

            place = _place(me, u, size)
            at = pl.multiple_of(place * unit, unit)
            here = pl.ds(at, unit)
            cos, sin = rotation(at)
            for n in range(g + 2):
                y = _dot(ab[...], w_s[:, n * block : (n + 1) * block], 1, 0).astype(BF16)
                for h in range(kv):
                    t = y[:, h * HEAD : (h + 1) * HEAD]
                    if n < g + 1:
                        t = t.astype(F32)
                        t = (t * cos + pltpu.roll(t, HEAD // 2, 1) * sin).astype(BF16)
                    if n < g:
                        head = n * kv + h
                        qc[place, head // g, (head % g) * unit : (head % g + 1) * unit, :] = t
                    else:
                        (kc if n == g else vc)[h, here, :] = t
                        (kt if n == g else vt)[h, :, here] = t.T

            chunk = lambda off: lax.rem(me + off, size)
            finished = lambda n: jnp.where(u == n, 1, 0)

            def diagonal(t, _):
                c = chunk(finished(5) * (size - 1 + 2 * t) + finished(7) * 2)
                forward(2 * c, c * big, unit, 0)
                forward(2 * c + 1, c * big, big, unit)

            def across(t, _):
                last = lax.div(t, 2)
                a = chunk(finished(5) * last * (size - 1) + finished(7) * 2)
                b = chunk(finished(5) * (size - 1 + 2 * lax.div(t + 1, 2)) + finished(7) * (lax.rem(t, 2) * (size - 1) + last))
                row, key = jnp.maximum(a, b), jnp.minimum(a, b)
                lax.fori_loop(0, 2, lambda n, _: forward(2 * row + n, key * big, big), None)

            lax.fori_loop(0, finished(1) + 2 * finished(5) + finished(7), diagonal, None)
            lax.fori_loop(0, 3 * finished(5) + 3 * finished(7), across, None)

        lax.fori_loop(0, units, one, None)
        pltpu.make_async_copy(ab, a_all.at[units - 1], out_sem.at[0]).wait()
        for stage in (0, 1):
            for c in own_copies(x_ref, x_all, x_send, x_recv, stage):
                c.wait_send()
        for c in passed_on(x_all, x_send, x_recv):
            c.wait_send()

    pl.run_scoped(project, pltpu.VMEM((d, (g + 2) * kv * HEAD), BF16), pltpu.VMEM((kv, big, cols), F32))
    for c in dy_loads:
        c.wait()
    wo_load.wait()

    def attend(dk_s, dv_s):
        dk_s[...] = jnp.zeros_like(dk_s)
        dv_s[...] = jnp.zeros_like(dv_s)

        def one(u, _):
            @pl.when(u == 2)
            def _():
                arrived(dyb, dy_send, dy_recv, 2)
                arrived(dyb, dy_send, dy_recv, 3)
                start(passed_on(dyb, dy_send, dy_recv))

            @pl.when(u >= 4)
            def _():
                arrived(dyb, dy_send, dy_recv, u)

            pltpu.make_async_copy(dyb.at[u], dy_all.at[u], out_sem.at[3]).start()
            block = 4 * HEAD
            for n in range(g * kv // 4):
                y = _dot(dyb[u], wo_s[n * block : (n + 1) * block, :], 1, 1).astype(BF16)
                for h in range(4):
                    head = n * 4 + h
                    doc[head // g, (head % g) * unit : (head % g + 1) * unit, :] = y[:, h * HEAD : (h + 1) * HEAD]

            place = _place(me, u, size)
            at = pl.multiple_of(place * unit, unit)
            whole = lax.div(place, 2)
            odd = lax.rem(place, 2)

            @pl.when(u >= 1)
            def _():
                pltpu.make_async_copy(o_st, o_all.at[u - 1], out_sem.at[1]).wait()
                pltpu.make_async_copy(dq_st, dq_all.at[u - 1], out_sem.at[2]).wait()

            def pair(hp, _):
                heads = [(i, hp * kb + i) for i in range(kb)]

                def gradients(here, lses, deltas, gap=None):
                    scores = [_dot(kc[h, here, :], qc[place, h], 1, 1) for i, h in heads]
                    dps = [_dot(vc[h, here, :], doc[h], 1, 1) for i, h in heads]
                    for i, h in heads:
                        p = jnp.exp2(scores[i] * e - lses[i])
                        if gap is not None:
                            p = jnp.where(mask(p.shape, gap), p, 0.0)
                        ds = (p * (dps[i] - deltas[i])).astype(BF16)
                        dv_s[h, here, :] += _dot(p.astype(BF16), doc[h], 1, 0)
                        dk_s[h, here, :] += _dot(ds, qc[place, h], 1, 0)
                        acc_dq[i] += _dot(kt[h, :, here], ds, 1, 0)

                small = lambda j: pl.ds(pl.multiple_of(at - j * unit, unit), unit)
                large = lambda j: pl.ds(pl.multiple_of(j * big, big), big)
                acc_dq[...] = jnp.zeros_like(acc_dq)
                for i, h in heads:
                    total = sum_s[place, pl.ds(h, 1), :]
                    out = (acc_o[place, h] * (1 / total)).astype(BF16).astype(F32)
                    row_s[i : i + 1, :] = top_s[place, pl.ds(h, 1), :] + jnp.log2(total)
                    row_s[kb + i : kb + i + 1, :] = (out * doc[h].astype(F32).T).sum(0, keepdims=True)
                    flat = out.T.astype(BF16)
                    for n in range(g):
                        o_st[:, _lanes(h * g + n, HEAD)] = flat[n * unit : (n + 1) * unit, :]
                lses = [row_s[i : i + 1, :] for i in range(kb)]
                deltas = [row_s[kb + i : kb + i + 1, :] for i in range(kb)]
                lax.fori_loop(0, whole, lambda j, _: gradients(large(j), lses, deltas), None)
                lax.fori_loop(0, odd + 1, lambda j, _: gradients(small(j), lses, deltas, j * unit), None)
                t = cs_ref[pl.ds(at, unit), :].T
                cos, sin = (jnp.concatenate([v] * g, 1) for v in (t[: HEAD // 2], t[HEAD // 2 :]))
                for i, h in heads:
                    dq = (acc_dq[i] * scale).astype(BF16).astype(F32)
                    a, b = dq[: HEAD // 2], dq[HEAD // 2 :]
                    flat = jnp.concatenate([a * cos + b * sin, b * cos - a * sin], 0).T.astype(BF16)
                    for n in range(g):
                        dq_st[:, _lanes(h * g + n, HEAD)] = flat[n * unit : (n + 1) * unit, :]

            lax.fori_loop(0, kv // kb, pair, None)
            pltpu.make_async_copy(o_st, o_all.at[u], out_sem.at[1]).start()
            pltpu.make_async_copy(dq_st, dq_all.at[u], out_sem.at[2]).start()
            pltpu.make_async_copy(dyb.at[u], dy_all.at[u], out_sem.at[3]).wait()

        lax.fori_loop(0, units, one, None)

        def last(u, _):
            at = pl.multiple_of(_place(me, u, size) * unit, unit)
            cos, sin = rotation(at)
            rows = pl.ds(pl.multiple_of(u * unit, unit), unit)
            for h in range(kv):
                dv_all[rows, h * HEAD : (h + 1) * HEAD] = dv_s[h, pl.ds(at, unit), :].astype(BF16)
                t = (dk_s[h, pl.ds(at, unit), :] * scale).astype(BF16).astype(F32)
                dk_all[rows, h * HEAD : (h + 1) * HEAD] = (t * cos - pltpu.roll(t, HEAD // 2, 1) * sin).astype(BF16)

        lax.fori_loop(0, units, last, None)

    every = units * unit
    pl.run_scoped(attend, pltpu.VMEM((kv, every, HEAD), F32), pltpu.VMEM((kv, every, HEAD), F32))
    pltpu.make_async_copy(o_st, o_all.at[units - 1], out_sem.at[1]).wait()
    pltpu.make_async_copy(dq_st, dq_all.at[units - 1], out_sem.at[2]).wait()
    for stage in (0, 1):
        for c in own_copies(dy_ref, dyb, dy_send, dy_recv, stage):
            c.wait_send()
    for c in passed_on(dyb, dy_send, dy_recv):
        c.wait_send()


def attention(x, dy, gain, wq, wk, wv, wo, cs, size):
    rows, d = x.shape
    unit, units = rows // 2, 2 * size
    nq, nk = wq.shape[1], wk.shape[1]
    kv, g = nk // HEAD, nq // nk
    every, cols = units * unit, g * unit
    anywhere, vmem = pl.BlockSpec(memory_space=pl.ANY), pl.BlockSpec(memory_space=pltpu.VMEM)
    in_hbm = lambda n: jax.ShapeDtypeStruct((units, unit, n), BF16)
    dma = pltpu.SemaphoreType.DMA
    return pl.pallas_call(
        functools.partial(_attention, size=size, g=g, scale=HEAD**-0.5),
        in_specs=[anywhere, anywhere, vmem, anywhere, anywhere, anywhere, anywhere, vmem],
        out_specs=[anywhere, anywhere, anywhere, vmem, anywhere, anywhere, vmem, vmem],
        out_shape=[in_hbm(d), in_hbm(d), in_hbm(d), jax.ShapeDtypeStruct((every, 1), F32), in_hbm(nq), in_hbm(nq),
                   jax.ShapeDtypeStruct((every, nk), BF16), jax.ShapeDtypeStruct((every, nk), BF16)],
        scratch_shapes=[
            pltpu.VMEM((units, unit, d), BF16), pltpu.VMEM((units, kv, cols, HEAD), BF16),
            pltpu.VMEM((kv, every, HEAD), BF16), pltpu.VMEM((kv, every, HEAD), BF16),
            pltpu.VMEM((kv, HEAD, every), BF16), pltpu.VMEM((kv, HEAD, every), BF16),
            pltpu.VMEM((nq, d), BF16), pltpu.VMEM((2, unit, d), BF16), pltpu.VMEM((unit, d), BF16),
            pltpu.VMEM((kv, cols, HEAD), BF16), pltpu.VMEM((unit, nq), BF16), pltpu.VMEM((unit, nq), BF16),
            pltpu.VMEM((units, kv, HEAD, cols), F32), pltpu.VMEM((2, HEAD, cols), F32),
            pltpu.VMEM((units, kv, cols), F32), pltpu.VMEM((units, kv, cols), F32), pltpu.VMEM((8, cols), F32),
            dma((units,)), dma((units,)), dma((units,)), dma((units,)), dma((6,)), dma((2,)), dma((5,)),
        ],
        compiler_params=pltpu.CompilerParams(collective_id=0, has_side_effects=True, vmem_limit_bytes=61 * 2**20),
        cost_estimate=pl.CostEstimate(flops=10**11, transcendentals=0, bytes_accessed=2**26),
        name="attention",
    )(x, dy, gain, wq, wk, wv, wo, cs)


def _normed_term(dq_ref, dk_ref, dv_ref, wq_ref, wk_ref, wv_ref, x_ref, inv_ref, g_ref, *out_refs):
    unit = out_refs[0].shape[0]
    by_gain = 0
    for n, ref in enumerate(out_refs):
        rows = slice(n * unit, (n + 1) * unit)
        t = _dot(dq_ref[n], wq_ref[...], 1, 1) + _dot(dk_ref[rows, :], wk_ref[...], 1, 1) + _dot(dv_ref[rows, :], wv_ref[...], 1, 1)
        ref[...] = t.astype(BF16)
        by_gain += (t * (x_ref[n].astype(F32) * inv_ref[rows, :])).sum(0, keepdims=True)
    g_ref[...] = by_gain


def normed_terms(dq, dk, dv, first, count, wq, wk, wv, x, inv, block=512):
    unit, nq, nk = dq.shape[1], wq.shape[1], wk.shape[1]
    d = wq.shape[0]
    at = first // count
    some = lambda w: pl.BlockSpec((count * unit, w), lambda i: (at, 0))
    row = lambda w: pl.BlockSpec((block, w), lambda i: (i, 0))
    column = lambda r: pl.BlockSpec((r, block), lambda i: (0, i))
    g, *out = pl.pallas_call(
        _normed_term,
        grid=(d // block,),
        in_specs=[pl.BlockSpec((count, unit, nq), lambda i: (at, 0, 0)), some(nk), some(nk), row(nq), row(nk), row(nk),
                  pl.BlockSpec((count, unit, block), lambda i: (at, 0, i)), some(1)],
        out_specs=[column(1)] + [column(unit)] * count,
        out_shape=[jax.ShapeDtypeStruct((1, d), F32)] + [jax.ShapeDtypeStruct((unit, d), BF16)] * count,
        compiler_params=pltpu.CompilerParams(dimension_semantics=("arbitrary",), vmem_limit_bytes=60 * 2**20),
        cost_estimate=pl.CostEstimate(flops=2 * count * unit * d * (nq + 2 * nk), transcendentals=0, bytes_accessed=2 * (count * unit + d) * (nq + 2 * nk) + 4 * count * unit * d),
        name="normed_terms",
    )(dq, dk, dv, wq, wk, wv, x, inv)
    return out, g


def _finish(x_ref, dy_ref, inv_ref, gain_ref, own_lo, l_lo, r_lo, own_hi, l_hi, r_hi, out_ref):
    for n, parts in enumerate(((own_lo, l_lo, r_lo), (own_hi, l_hi, r_hi))):
        t = (parts[0][...].astype(F32) + parts[1][...].astype(F32) + parts[2][...].astype(F32)) * gain_ref[...].astype(F32)
        inv = inv_ref[n]
        hat = x_ref[n].astype(F32) * inv
        out_ref[n] = (dy_ref[n].astype(F32) + inv * (t - hat * jnp.mean(t * hat, -1, keepdims=True))).astype(BF16)


def finish(x, dy, inv, gain, lo, hi, block=64):
    rows, d = x.shape
    unit = rows // 2
    both = lambda w: pl.BlockSpec((2, block, w), lambda i: (0, i, 0))
    halves = lambda t: t.reshape(2, unit, -1)
    return pl.pallas_call(
        _finish,
        grid=(unit // block,),
        in_specs=[both(d), both(d), both(1), pl.BlockSpec((1, d), lambda i: (0, 0))] + [pl.BlockSpec((block, d), lambda i: (i, 0))] * 6,
        out_specs=both(d),
        out_shape=jax.ShapeDtypeStruct((2, unit, d), BF16),
        compiler_params=pltpu.CompilerParams(dimension_semantics=("arbitrary",), vmem_limit_bytes=32 * 2**20),
        cost_estimate=pl.CostEstimate(flops=10 * rows * d, transcendentals=0, bytes_accessed=12 * rows * d),
        name="finish",
    )(halves(x), halves(dy), halves(inv), gain, *lo, *hi).reshape(rows, d)


def angles(rows):
    n = HEAD // 2
    angle = np.arange(rows, dtype=np.float32)[:, None] * np.float32(THETA) ** (-np.arange(n, dtype=np.float32) / np.float32(n))
    angle = angle.astype(np.float64)
    return np.concatenate([np.cos(angle), np.sin(angle)], 1).astype(np.float32)


def solution(mesh):
    size = mesh.shape["tp"]
    to_right = [(i, (i + 1) % size) for i in range(size)]
    to_left = [(i, (i - 1) % size) for i in range(size)]

    def right(t):
        return lax.ppermute(t, "tp", to_right)

    def left(t):
        return lax.ppermute(t, "tp", to_left)

    def program(x, dy, gain, wq, wk, wv, wo):
        rows = x.shape[0]
        x_all, dy_all, a_all, inv, o_all, dq, dk, dv = attention(x, dy, gain[None], wq, wk, wv, wo, jnp.asarray(angles(size * rows)), size)

        def after(first, *rest):
            return lax.optimization_barrier((first, *rest))[1:]

        add = lambda t, got: (t.astype(F32) + got.astype(F32)).astype(BF16)
        (opp_lo, opp_hi), g_opp = normed_terms(dq, dk, dv, 6, 2, wq, wk, wv, x_all, inv)
        o_lo = right(opp_lo)
        o_hi = left(opp_hi)
        dq, dk = after(opp_lo, dq, dk)
        (own_lo, own_hi, lf_lo, rt_hi, lf_hi, rt_lo), g_rest = normed_terms(dq, dk, dv, 0, 6, wq, wk, wv, x_all, inv)
        from_l_hi = right(rt_hi)
        from_r_lo = left(lf_lo)
        gs = g_opp + g_rest
        ring = [gs, left(gs), lax.ppermute(gs, "tp", [(i, (i + 2) % size) for i in range(size)]), right(gs)]
        ring = jnp.roll(jnp.stack(ring), lax.axis_index("tp"), 0)
        by_gain = functools.reduce(jnp.add, [ring[i] for i in range(size)])

        flat = lambda t: t.reshape(-1, t.shape[-1])
        (o_all,) = after(own_lo, o_all)
        by_wo = _dot(flat(o_all), flat(dy_all), 0, 0).astype(BF16)
        o_lo, o_hi = after(by_wo, o_lo, o_hi)
        to_r, to_l = add(rt_lo, o_lo), add(lf_hi, o_hi)
        from_l_lo = right(to_r)
        from_r_hi = left(to_l)
        _, a_all = after(to_r, to_l, flat(a_all))
        by_wq = _dot(a_all, flat(dq), 0, 0).astype(BF16)
        by_wk = _dot(a_all, dk, 0, 0).astype(BF16)
        by_wv = _dot(a_all, dv, 0, 0).astype(BF16)
        by_x = finish(x, dy, inv[:rows], gain[None], (own_lo, from_l_lo, from_r_lo), (own_hi, from_l_hi, from_r_hi))
        return by_x, by_gain, by_wq, by_wk, by_wv, by_wo

    tokens, columns = P(("dp", "tp"), None), P(None, "tp")
    return jax.shard_map(
        program,
        mesh=mesh,
        in_specs=(tokens, tokens, P(None), columns, columns, columns, P("tp", None)),
        out_specs=(tokens, P("dp", None), P("dp", "tp"), P("dp", "tp"), P("dp", "tp"), P(("dp", "tp"), None)),
        check_vma=False,
    )
```

```python
import functools

import jax
import jax.numpy as jnp
import numpy as np
from jax import lax
from jax.experimental import pallas as pl
from jax.experimental.pallas import tpu as pltpu
from jax.sharding import PartitionSpec as P


HEAD = 128
THETA = 10000
LOG2E = 1.4426950408889634
NEG = -1e30
HIDDEN = -2e30
F32, BF16 = jnp.float32, jnp.bfloat16


def _dot(a, b, ca, cb):
    return lax.dot_general(a, b, (((ca,), (cb,)), ((), ())), preferred_element_type=F32)


MESH = pl.DeviceIdType.MESH


def _place(me, u, size):
    group, b = lax.div(u, 2), lax.rem(u, 2)
    middle = lax.rem(lax.div(group + 1, 2), 2)
    end = lax.div(group, 3)
    off = middle * (size - 1 + 2 * b) + end * 2
    half = middle * (group - 1) + (1 - middle) * b
    return lax.rem(me + off, size) * 2 + half


def _lanes(h, width):
    return pl.ds(pl.multiple_of(h * width, width), width)


def _attention(x_ref, dy_ref, gain_ref, wq_ref, wk_ref, wv_ref, wo_ref, cs_ref,
               x_all, dy_all, at_all, inv_all, ot_all, dq_all, dk_all, dv_all,
               dyb, qc, kc, vc, kt, vt, wo_s, xb, ab, at_st, doc, o_st, dq_st, acc_o, acc_dq, top_s, sum_s, row_s,
               x_send, x_recv, dy_send, dy_recv, w_sem, load_sem, out_sem, *, size, g, scale):
    unit, d = ab.shape
    kv = kc.shape[0]
    units = 2 * size
    kb = 2
    cols = g * unit
    e = scale * LOG2E
    me = lax.axis_index("tp")
    right = {"tp": lax.rem(me + 1, size)}
    left = {"tp": lax.rem(me + size - 1, size)}

    barrier = pltpu.get_barrier_semaphore()
    for other in (left, right):
        pl.semaphore_signal(barrier, inc=1, device_id=other, device_id_type=MESH)
    pl.semaphore_wait(barrier, 2)

    def half(ref, n):
        return ref.at[pl.ds(n * unit, unit), :]

    def remote(source, target, send, recv, u, other):
        return pltpu.make_async_remote_copy(src_ref=source, dst_ref=target.at[u], send_sem=send.at[u], recv_sem=recv.at[u], device_id=other, device_id_type=MESH)

    def own_copies(ref, target, send, recv, stage):
        n = 2 + 2 * stage
        return (remote(half(ref, stage), target, send, recv, n, right), remote(half(ref, stage), target, send, recv, n + 1, left))

    def passed_on(target, send, recv, stage):
        copies = []
        for n, other in enumerate((right, left)):
            part = pl.ds(n * (unit // 2), unit // 2)
            k = 6 + 2 * stage + n
            copies.append(pltpu.make_async_remote_copy(
                src_ref=target.at[2 + 2 * stage + n, part, :], dst_ref=target.at[6 + stage, part, :], send_sem=send.at[k], recv_sem=recv.at[k],
                device_id=other, device_id_type=MESH))
        return copies

    def both_arrived(target, send, recv, stage):
        for c in passed_on(target, send, recv, stage):
            c.wait_recv()

    def out_copy(ref, target, u, sem):
        return pltpu.make_async_copy(ref, target.at[:, pl.ds(u * unit if isinstance(u, int) else pl.multiple_of(u * unit, unit), unit)], out_sem.at[sem])

    def start(copies):
        for c in copies:
            c.start()

    for stage in (0, 1):
        start(own_copies(x_ref, x_all, x_send, x_recv, stage))
    dy_loads = [pltpu.make_async_copy(half(dy_ref, n), dyb.at[n], w_sem.at[4 + n]) for n in range(2)]
    wo_load = pltpu.make_async_copy(wo_ref, wo_s, w_sem.at[3])

    def arrived(target, send, recv, u):
        remote(target.at[2], target, send, recv, u, right).wait_recv()

    def rotation(at):
        t = cs_ref[pl.ds(at, unit), :]
        low = lax.broadcasted_iota(jnp.int32, t.shape, 1) < HEAD // 2
        turned = pltpu.roll(t, HEAD // 2, 1)
        return jnp.where(low, t, turned), jnp.where(low, -turned, t)

    big = 2 * unit
    top_s[...] = jnp.full_like(top_s, NEG)
    sum_s[...] = jnp.zeros_like(sum_s)
    acc_o[...] = jnp.zeros_like(acc_o)

    def mask(shape, gap):
        return lax.rem(lax.broadcasted_iota(jnp.int32, shape, 1), unit) + gap >= lax.broadcasted_iota(jnp.int32, shape, 0)

    def by_seen(u, slot):
        block = 4 * HEAD
        for n in range(g * kv // 4):
            y = _dot(dyb[u], wo_s[n * block : (n + 1) * block, :], 1, 1).astype(BF16)
            for h in range(4):
                head = n * 4 + h
                doc[slot, head // g, (head % g) * unit : (head % g + 1) * unit, :] = y[:, h * HEAD : (h + 1) * HEAD]

    def project(w_s, s_s):
        loads, at = [], 0
        for n, ref in enumerate((wq_ref, wk_ref, wv_ref)):
            loads.append(pltpu.make_async_copy(ref, w_s.at[:, pl.ds(at, ref.shape[1])], w_sem.at[n]))
            at += ref.shape[1]
        start(loads)
        start(dy_loads)
        wo_load.start()
        block = kv * HEAD

        def forward(row, at, n, gap=None):
            here = pl.ds(pl.multiple_of(at, n), n)
            tops = {}
            for h in range(kv + 1):
                if h < kv:
                    s = _dot(kc[h, here, :], qc[row, h], 1, 1) * e
                    if gap is not None:
                        s = jnp.where(mask(s.shape, gap), s, HIDDEN)
                    s_s[h, :n, :] = s
                    old = top_s[row, h : h + 1, :]
                    tops[h] = old, jnp.maximum(old, s.max(0, keepdims=True))
                    top_s[row, h : h + 1, :] = tops[h][1]
                if h:
                    i = h - 1
                    old, top = tops[i]
                    keep = jnp.exp2(old - top)
                    p = jnp.exp2(s_s[i, :n, :] - top)
                    sum_s[row, i : i + 1, :] = sum_s[row, i : i + 1, :] * keep + p.sum(0, keepdims=True)
                    acc_o[row, i] = acc_o[row, i] * keep + _dot(vt[i, :, here], p.astype(BF16), 1, 0)

        def at_copy(u):
            n = u % 2 if isinstance(u, int) else lax.rem(u, 2)
            return out_copy(at_st.at[n], at_all, u, 5 * n)

        def own_out(u):
            return pltpu.make_async_copy(xb.at[u], x_all.at[u], out_sem.at[4 + 2 * u])

        def one(u, _):
            @pl.when(u == 2)
            def _():
                own_out(0).wait()
                own_out(1).wait()

            @pl.when(lax.rem(u, 2) == 0)
            def _():
                @pl.when((u >= 2) & (u < 6))
                def _():
                    for n in range(2):
                        arrived(x_all, x_send, x_recv, u + n)
                        pltpu.make_async_copy(x_all.at[u + n], xb.at[n], load_sem.at[n]).start()

                @pl.when(u < 2)
                def _():
                    for n in range(2):
                        pltpu.make_async_copy(half(x_ref, n), xb.at[n], load_sem.at[n]).start()

            for stage in (0, 1):
                @pl.when(u == 2 + 2 * stage)
                def _():
                    start(passed_on(x_all, x_send, x_recv, stage))

                @pl.when(u == 6 + stage)
                def _():
                    both_arrived(x_all, x_send, x_recv, stage)
                    pltpu.make_async_copy(x_all.at[6 + stage], xb.at[stage], load_sem.at[stage]).start()

            @pl.when(u == 4)
            def _():
                for stage in (0, 1):
                    start(own_copies(dy_ref, dyb, dy_send, dy_recv, stage))

            now = lax.rem(u, 2)
            pltpu.make_async_copy(x_all.at[u], xb.at[now], load_sem.at[now]).wait()

            @pl.when(u < 2)
            def _():
                own_out(u).start()

            @pl.when(u >= 2)
            def _():
                at_copy(u - 2).wait()

            wide = xb[now].astype(F32)
            inv = lax.rsqrt(jnp.mean(wide * wide, -1, keepdims=True) + 1e-6)
            rows = pl.ds(pl.multiple_of(u * unit, unit), unit)
            inv_all[rows, :] = inv
            ab[...] = (wide * inv * gain_ref[...].astype(F32)[None]).astype(BF16)
            at_st[now] = ab[...].T
            at_copy(u).start()

            @pl.when(u == 0)
            def _():
                for c in loads:
                    c.wait()

            place = _place(me, u, size)
            at = pl.multiple_of(place * unit, unit)
            here = pl.ds(at, unit)
            cos, sin = rotation(at)
            for n in range(g + 2):
                y = _dot(ab[...], w_s[:, n * block : (n + 1) * block], 1, 0).astype(BF16)
                for h in range(kv):
                    t = y[:, h * HEAD : (h + 1) * HEAD]
                    if n < g + 1:
                        t = t.astype(F32)
                        t = (t * cos + pltpu.roll(t, HEAD // 2, 1) * sin).astype(BF16)
                    if n < g:
                        head = n * kv + h
                        qc[place, head // g, (head % g) * unit : (head % g + 1) * unit, :] = t
                    else:
                        (kc if n == g else vc)[h, here, :] = t
                        (kt if n == g else vt)[h, :, here] = t.T

            @pl.when(u == 3)
            def _():
                for c in dy_loads:
                    c.wait()
                wo_load.wait()
                lax.fori_loop(0, 2, lambda n, _: by_seen(n, n), None)

            chunk = lambda off: lax.rem(me + off, size)
            finished = lambda n: jnp.where(u == n, 1, 0)

            def diagonal(t, _):
                c = chunk(finished(5) * (size - 1 + 2 * t) + finished(7) * 2)
                forward(2 * c, c * big, unit, 0)
                forward(2 * c + 1, c * big, big, unit)

            def across(t, _):
                last = lax.div(t, 2)
                a = chunk(finished(5) * last * (size - 1) + finished(7) * 2)
                b = chunk(finished(5) * (size - 1 + 2 * lax.div(t + 1, 2)) + finished(7) * (lax.rem(t, 2) * (size - 1) + last))
                row, key = jnp.maximum(a, b), jnp.minimum(a, b)
                lax.fori_loop(0, 2, lambda n, _: forward(2 * row + n, key * big, big), None)

            lax.fori_loop(0, finished(1) + 2 * finished(5) + finished(7), diagonal, None)
            lax.fori_loop(0, 3 * finished(5) + 3 * finished(7), across, None)

        lax.fori_loop(0, units, one, None)
        at_copy(units - 2).wait()
        at_copy(units - 1).wait()
        for stage in (0, 1):
            for c in own_copies(x_ref, x_all, x_send, x_recv, stage):
                c.wait_send()
            for c in passed_on(x_all, x_send, x_recv, stage):
                c.wait_send()

    pl.run_scoped(project, pltpu.VMEM((d, (g + 2) * kv * HEAD), BF16), pltpu.VMEM((kv, big, cols), F32))

    def attend(dk_s, dv_s):
        dk_s[...] = jnp.zeros_like(dk_s)
        dv_s[...] = jnp.zeros_like(dv_s)

        def one(u, _):
            for stage in (0, 1):
                @pl.when(u == 2 + 2 * stage)
                def _():
                    arrived(dyb, dy_send, dy_recv, 2 + 2 * stage)
                    arrived(dyb, dy_send, dy_recv, 3 + 2 * stage)
                    start(passed_on(dyb, dy_send, dy_recv, stage))

                @pl.when(u == 6 + stage)
                def _():
                    both_arrived(dyb, dy_send, dy_recv, stage)

            pltpu.make_async_copy(dyb.at[u], dy_all.at[u], out_sem.at[3]).start()

            @pl.when(u >= 2)
            def _():
                by_seen(u, 2)

            slot = jnp.minimum(u, 2)
            place = _place(me, u, size)
            at = pl.multiple_of(place * unit, unit)
            whole = lax.div(place, 2)
            odd = lax.rem(place, 2)

            @pl.when(u >= 1)
            def _():
                out_copy(o_st, ot_all, u - 1, 1).wait()
                pltpu.make_async_copy(dq_st, dq_all.at[u - 1], out_sem.at[2]).wait()

            def pair(hp, _):
                heads = [(i, hp * kb + i) for i in range(kb)]

                def gradients(here, lses, deltas, gap=None):
                    scores = [_dot(kc[h, here, :], qc[place, h], 1, 1) for i, h in heads]
                    dps = [_dot(vc[h, here, :], doc[slot, h], 1, 1) for i, h in heads]
                    for i, h in heads:
                        p = jnp.exp2(scores[i] * e - lses[i])
                        if gap is not None:
                            p = jnp.where(mask(p.shape, gap), p, 0.0)
                        ds = (p * (dps[i] - deltas[i])).astype(BF16)
                        dv_s[h, here, :] += _dot(p.astype(BF16), doc[slot, h], 1, 0)
                        dk_s[h, here, :] += _dot(ds, qc[place, h], 1, 0)
                        acc_dq[i] += _dot(kt[h, :, here], ds, 1, 0)

                large = lambda j: pl.ds(pl.multiple_of(j * big, big), big)
                acc_dq[...] = jnp.zeros_like(acc_dq)
                for i, h in heads:
                    total = sum_s[place, pl.ds(h, 1), :]
                    out = (acc_o[place, h] * (1 / total)).astype(BF16).astype(F32)
                    row_s[i : i + 1, :] = top_s[place, pl.ds(h, 1), :] + jnp.log2(total)
                    row_s[kb + i : kb + i + 1, :] = (out * doc[slot, h].astype(F32).T).sum(0, keepdims=True)
                    for n in range(g):
                        o_st[_lanes(h * g + n, HEAD), :] = out[:, n * unit : (n + 1) * unit].astype(BF16)
                lses = [row_s[i : i + 1, :] for i in range(kb)]
                deltas = [row_s[kb + i : kb + i + 1, :] for i in range(kb)]
                lax.fori_loop(0, whole, lambda j, _: gradients(large(j), lses, deltas), None)

                @pl.when(odd == 1)
                def _():
                    gradients(large(whole), lses, deltas, unit)

                @pl.when(odd == 0)
                def _():
                    gradients(pl.ds(at, unit), lses, deltas, 0)

                t = cs_ref[pl.ds(at, unit), :].T
                cos, sin = (jnp.concatenate([v] * g, 1) for v in (t[: HEAD // 2], t[HEAD // 2 :]))
                for i, h in heads:
                    dq = (acc_dq[i] * scale).astype(BF16).astype(F32)
                    a, b = dq[: HEAD // 2], dq[HEAD // 2 :]
                    flat = jnp.concatenate([a * cos + b * sin, b * cos - a * sin], 0).astype(BF16).T
                    for n in range(g):
                        dq_st[:, _lanes(h * g + n, HEAD)] = flat[n * unit : (n + 1) * unit, :]

            lax.fori_loop(0, kv // kb, pair, None)
            out_copy(o_st, ot_all, u, 1).start()
            pltpu.make_async_copy(dq_st, dq_all.at[u], out_sem.at[2]).start()
            pltpu.make_async_copy(dyb.at[u], dy_all.at[u], out_sem.at[3]).wait()

        lax.fori_loop(0, units, one, None)

        def last(u, _):
            at = pl.multiple_of(_place(me, u, size) * unit, unit)
            cos, sin = rotation(at)
            rows = pl.ds(pl.multiple_of(u * unit, unit), unit)
            for h in range(kv):
                dv_all[rows, h * HEAD : (h + 1) * HEAD] = dv_s[h, pl.ds(at, unit), :].astype(BF16)
                t = (dk_s[h, pl.ds(at, unit), :] * scale).astype(BF16).astype(F32)
                dk_all[rows, h * HEAD : (h + 1) * HEAD] = (t * cos - pltpu.roll(t, HEAD // 2, 1) * sin).astype(BF16)

        lax.fori_loop(0, units, last, None)

    every = units * unit
    pl.run_scoped(attend, pltpu.VMEM((kv, every, HEAD), F32), pltpu.VMEM((kv, every, HEAD), F32))
    out_copy(o_st, ot_all, units - 1, 1).wait()
    pltpu.make_async_copy(dq_st, dq_all.at[units - 1], out_sem.at[2]).wait()
    for stage in (0, 1):
        for c in own_copies(dy_ref, dyb, dy_send, dy_recv, stage):
            c.wait_send()
        for c in passed_on(dyb, dy_send, dy_recv, stage):
            c.wait_send()


def attention(x, dy, gain, wq, wk, wv, wo, cs, size):
    rows, d = x.shape
    unit, units = rows // 2, 2 * size
    nq, nk = wq.shape[1], wk.shape[1]
    kv, g = nk // HEAD, nq // nk
    every, cols = units * unit, g * unit
    anywhere, vmem = pl.BlockSpec(memory_space=pl.ANY), pl.BlockSpec(memory_space=pltpu.VMEM)
    in_hbm = lambda n: jax.ShapeDtypeStruct((units, unit, n), BF16)
    dma = pltpu.SemaphoreType.DMA
    return pl.pallas_call(
        functools.partial(_attention, size=size, g=g, scale=HEAD**-0.5),
        in_specs=[anywhere, anywhere, vmem, anywhere, anywhere, anywhere, anywhere, vmem],
        out_specs=[anywhere, anywhere, anywhere, vmem, anywhere, anywhere, vmem, vmem],
        out_shape=[in_hbm(d), in_hbm(d), jax.ShapeDtypeStruct((d, every), BF16), jax.ShapeDtypeStruct((every, 1), F32), jax.ShapeDtypeStruct((nq, every), BF16), in_hbm(nq),
                   jax.ShapeDtypeStruct((every, nk), BF16), jax.ShapeDtypeStruct((every, nk), BF16)],
        scratch_shapes=[
            pltpu.VMEM((units, unit, d), BF16), pltpu.VMEM((units, kv, cols, HEAD), BF16),
            pltpu.VMEM((kv, every, HEAD), BF16), pltpu.VMEM((kv, every, HEAD), BF16),
            pltpu.VMEM((kv, HEAD, every), BF16), pltpu.VMEM((kv, HEAD, every), BF16),
            pltpu.VMEM((nq, d), BF16), pltpu.VMEM((2, unit, d), BF16), pltpu.VMEM((unit, d), BF16), pltpu.VMEM((2, d, unit), BF16),
            pltpu.VMEM((3, kv, cols, HEAD), BF16), pltpu.VMEM((nq, unit), BF16), pltpu.VMEM((unit, nq), BF16),
            pltpu.VMEM((units, kv, HEAD, cols), F32), pltpu.VMEM((2, HEAD, cols), F32),
            pltpu.VMEM((units, kv, cols), F32), pltpu.VMEM((units, kv, cols), F32), pltpu.VMEM((8, cols), F32),
            *[dma((units + 2,))] * 4, dma((6,)), dma((2,)), dma((7,)),
        ],
        compiler_params=pltpu.CompilerParams(collective_id=0, has_side_effects=True, vmem_limit_bytes=63 * 2**20),
        cost_estimate=pl.CostEstimate(flops=10**11, transcendentals=0, bytes_accessed=2**26),
        name="attention",
    )(x, dy, gain, wq, wk, wv, wo, cs)


LIMITS = {2: 60 * 2**20, 6: 60 * 2**20}


def _normed_term(dq_ref, dk_ref, dv_ref, wq_ref, wk_ref, wv_ref, x_ref, inv_ref, g_ref, *out_refs):
    unit = out_refs[0].shape[0]
    dq = dq_ref[...].reshape(dk_ref.shape[0], -1)
    every = _dot(dq, wq_ref[...], 1, 1) + _dot(dk_ref[...], wk_ref[...], 1, 1) + _dot(dv_ref[...], wv_ref[...], 1, 1)
    by_gain = 0
    for n, ref in enumerate(out_refs):
        rows = slice(n * unit, (n + 1) * unit)
        t = every[rows]
        ref[...] = t.astype(BF16)
        by_gain += (t * (x_ref[n].astype(F32) * inv_ref[rows, :])).sum(0, keepdims=True)
    g_ref[...] = by_gain


def normed_terms(dq, dk, dv, first, count, wq, wk, wv, x, inv, block=512):
    unit, nq, nk = dq.shape[1], wq.shape[1], wk.shape[1]
    d = wq.shape[0]
    at = first // count
    some = lambda w: pl.BlockSpec((count * unit, w), lambda i: (at, 0))
    row = lambda w: pl.BlockSpec((block, w), lambda i: (i, 0))
    column = lambda r: pl.BlockSpec((r, block), lambda i: (0, i))
    g, *out = pl.pallas_call(
        _normed_term,
        grid=(d // block,),
        in_specs=[pl.BlockSpec((count, unit, nq), lambda i: (at, 0, 0)), some(nk), some(nk), row(nq), row(nk), row(nk),
                  pl.BlockSpec((count, unit, block), lambda i: (at, 0, i)), some(1)],
        out_specs=[column(1)] + [column(unit)] * count,
        out_shape=[jax.ShapeDtypeStruct((1, d), F32)] + [jax.ShapeDtypeStruct((unit, d), BF16)] * count,
        compiler_params=pltpu.CompilerParams(dimension_semantics=("arbitrary",), vmem_limit_bytes=LIMITS[count]),
        cost_estimate=pl.CostEstimate(flops=2 * count * unit * d * (nq + 2 * nk), transcendentals=0, bytes_accessed=2 * (count * unit + d) * (nq + 2 * nk) + 4 * count * unit * d),
        name="normed_terms",
    )(dq, dk, dv, wq, wk, wv, x, inv)
    return out, g


def _finish(x_ref, dy_ref, inv_ref, gain_ref, own_lo, l_lo, r_lo, own_hi, l_hi, r_hi, out_ref):
    for n, parts in enumerate(((own_lo, l_lo, r_lo), (own_hi, l_hi, r_hi))):
        t = (parts[0][...].astype(F32) + parts[1][...].astype(F32) + parts[2][...].astype(F32)) * gain_ref[...].astype(F32)
        inv = inv_ref[n]
        hat = x_ref[n].astype(F32) * inv
        out_ref[n] = (dy_ref[n].astype(F32) + inv * (t - hat * jnp.mean(t * hat, -1, keepdims=True))).astype(BF16)


def finish(x, dy, inv, gain, lo, hi, block=64):
    rows, d = x.shape
    unit = rows // 2
    both = lambda w: pl.BlockSpec((2, block, w), lambda i: (0, i, 0))
    halves = lambda t: t.reshape(2, unit, -1)
    return pl.pallas_call(
        _finish,
        grid=(unit // block,),
        in_specs=[both(d), both(d), both(1), pl.BlockSpec((1, d), lambda i: (0, 0))] + [pl.BlockSpec((block, d), lambda i: (i, 0))] * 6,
        out_specs=both(d),
        out_shape=jax.ShapeDtypeStruct((2, unit, d), BF16),
        compiler_params=pltpu.CompilerParams(dimension_semantics=("arbitrary",), vmem_limit_bytes=32 * 2**20),
        cost_estimate=pl.CostEstimate(flops=10 * rows * d, transcendentals=0, bytes_accessed=12 * rows * d),
        name="finish",
    )(halves(x), halves(dy), halves(inv), gain, *lo, *hi).reshape(rows, d)


def angles(rows):
    n = HEAD // 2
    angle = np.arange(rows, dtype=np.float32)[:, None] * np.float32(THETA) ** (-np.arange(n, dtype=np.float32) / np.float32(n))
    angle = angle.astype(np.float64)
    return np.concatenate([np.cos(angle), np.sin(angle)], 1).astype(np.float32)


def solution(mesh):
    size = mesh.shape["tp"]
    to_right = [(i, (i + 1) % size) for i in range(size)]
    to_left = [(i, (i - 1) % size) for i in range(size)]

    def right(t):
        return lax.ppermute(t, "tp", to_right)

    def left(t):
        return lax.ppermute(t, "tp", to_left)

    def program(x, dy, gain, wq, wk, wv, wo):
        rows = x.shape[0]
        x_all, dy_all, a_t, inv, o_t, dq, dk, dv = attention(x, dy, gain, wq, wk, wv, wo, jnp.asarray(angles(size * rows)), size)

        def after(first, *rest):
            return lax.optimization_barrier((first, *rest))[1:]

        add = lambda t, got: (t.astype(F32) + got.astype(F32)).astype(BF16)
        (opp_lo, opp_hi), g_opp = normed_terms(dq, dk, dv, 6, 2, wq, wk, wv, x_all, inv)
        o_lo = right(opp_lo)
        o_hi = left(opp_hi)
        dq, dk = after(opp_lo, dq, dk)
        (own_lo, own_hi, lf_lo, rt_lo, lf_hi, rt_hi), g_rest = normed_terms(dq, dk, dv, 0, 6, wq, wk, wv, x_all, inv)
        from_l_hi = right(rt_hi)
        from_r_lo = left(lf_lo)
        gs = g_opp + g_rest
        ring = [gs, left(gs), lax.ppermute(gs, "tp", [(i, (i + 2) % size) for i in range(size)]), right(gs)]
        ring = jnp.roll(jnp.stack(ring), lax.axis_index("tp"), 0)
        by_gain = functools.reduce(jnp.add, [ring[i] for i in range(size)])

        flat = lambda t: t.reshape(-1, t.shape[-1])
        (o_t,) = after(own_lo, o_t)
        by_wo = _dot(o_t, flat(dy_all), 1, 0).astype(BF16)
        o_lo, o_hi = after(by_wo, o_lo, o_hi)
        to_r, to_l = add(rt_lo, o_lo), add(lf_hi, o_hi)
        from_l_lo = right(to_r)
        from_r_hi = left(to_l)
        _, a_t = after(to_r, to_l, a_t)
        by_wq = _dot(a_t, flat(dq), 1, 0).astype(BF16)
        by_wk = _dot(a_t, dk, 1, 0).astype(BF16)
        by_wv = _dot(a_t, dv, 1, 0).astype(BF16)
        by_x = finish(x, dy, inv[:rows], gain[None], (own_lo, from_l_lo, from_r_lo), (own_hi, from_l_hi, from_r_hi))
        return by_x, by_gain, by_wq, by_wk, by_wv, by_wo

    tokens, columns = P(("dp", "tp"), None), P(None, "tp")
    return jax.shard_map(
        program,
        mesh=mesh,
        in_specs=(tokens, tokens, P(None), columns, columns, columns, P("tp", None)),
        out_specs=(tokens, P("dp", None), P("dp", "tp"), P("dp", "tp"), P("dp", "tp"), P(("dp", "tp"), None)),
        check_vma=False,
    )
```
